256 devices in a mesh: cand: 16 (over z_hi, x, core), seq: 16 (over z_lo, y).
Axes of the slice: x: 4, y: 4, z: 8 (z_hi: 2, z_lo: 4; z = z_hi * 4 + z_lo), core: 2. Of those that a mesh axis runs over, the one named last changes fastest.
Arguments:
- latent: bfloat16 [16, 768, 3072], P('cand', 'seq'), may hold values from -0.59765625 to 0.59765625
- timesteps: int32 [16], replicated, may hold values from 0 to 999
- positions: int32 [3, 768], replicated, may hold values from 0 to 63
- mod_weight: bfloat16 [3072, 9216], P('cand', 'seq'), may hold values from -0.109375 to 0.109375
- input_weight: bfloat16 [3072, 16, 384], P('cand', 'seq'), may hold values from -0.109375 to 0.109375
- output_weight: bfloat16 [16, 128, 3072], P('seq', None, 'cand'), may hold values from -0.75 to 0.75
- cotangent: bfloat16 [16, 768, 3072], P('cand', 'seq'), may hold values from -6 to 6
Outputs:
- block_out: bfloat16 [16, 768, 3072], P('cand', 'seq')
- latent_grad: float32 [16, 768, 3072], P('cand', 'seq')
The draws below stay inside these ranges and needn't reach their ends.
All inputs are finite; a program needn't handle non-finite values.
Results may differ from the reference program's by a relative error of at most 0.033.
Values may be sent and summed in bfloat16 or wider, within the bound.
No kernel may reach another device: no remote copies, remote signals or barrier semaphores. Data moves between devices by JAX's collectives and lax.ppermute only.
A program may use at most 128 MiB of HBM per device.

```python
import jax
import jax.numpy as jnp
import numpy as np
from jax import lax

D = 3072
HEADS = 16
HEAD = 128
LEN = 768
CANDS = 16
GROUP = 1
ATT_WIDTH = 2048
N_SEQ = 16


def with_ends(drawn, stream_key, low, top_value):
    extent = drawn.shape
    place = [jax.random.randint(jax.random.fold_in(stream_key, axis), (), 0, extent[axis]) for axis in range(len(extent))]
    drawn = drawn.at[tuple(place)].set(low)
    longest = extent.index(max(extent))
    place[longest] = (place[longest] + 1) % extent[longest]
    return drawn.at[tuple(place)].set(top_value)


def levels(rng, shape, shards, low, largest):
    def one(axis_at, blocks):
        steps = jax.random.uniform(jax.random.fold_in(jax.random.fold_in(rng, 6), axis_at), (blocks,), jnp.float32, low / len(shards), largest / len(shards))
        return jnp.repeat(jnp.exp(steps), shape[axis_at] // blocks).reshape((-1,) + (1,) * (len(shape) - axis_at - 1))

    loudness = one(*shards[0])
    for cut in shards[1:]:
        loudness = loudness * one(*cut)
    return loudness


def scatter_about(key, extent, spread, bound, cuts=(), kind=jnp.bfloat16):
    loudness = levels(key, extent, cuts, -0.22, 0.18) if cuts else 1.0
    entries = jax.random.normal(key, extent, jnp.float32) * spread * loudness
    return jnp.minimum(jnp.maximum(entries, -bound), bound).astype(kind)


def setup_inputs(seed: int = 0) -> dict:
    arg_keys = jax.random.split(jax.random.key(seed), 8)
    return {
        "latent": scatter_about(arg_keys[0], (CANDS, LEN, D), 0.1, 0.59765625, ((0, 16), (1, 16))),
        "timesteps": with_ends(jax.random.randint(arg_keys[1], (CANDS,), 0, 1000), jax.random.fold_in(arg_keys[1], 1), 0, 999).astype(jnp.int32),
        "positions": with_ends(jax.random.randint(arg_keys[2], (3, LEN), 0, 64), jax.random.fold_in(arg_keys[2], 1), 0, 63).astype(jnp.int32),
        "mod_weight": scatter_about(arg_keys[3], (D, 3 * D), D ** -0.5, 0.109375, ((0, 16), (1, 16))),
        "input_weight": scatter_about(arg_keys[4], (D, HEADS, 3 * HEAD), D ** -0.5, 0.109375, ((0, 16), (1, 16))),
        "output_weight": scatter_about(arg_keys[5], (HEADS, HEAD, D), (ATT_WIDTH // 32) ** -0.5, 0.75, ((0, 16), (2, 16))),
        "cotangent": scatter_about(arg_keys[6], (CANDS, LEN, D), 1.0, 6.0, ((0, 16), (1, 16))),
    }


epsilon = 1e-06

def time_embed(timesteps, feature_width):
    half_size = feature_width // 2
    freq_rate = jnp.exp(-jnp.log(10000.0) * jnp.arange(half_size, dtype=jnp.float32) / half_size)
    angles = timesteps.astype(jnp.float32)[:, None] * freq_rate[None, :]
    return jnp.concatenate([jnp.cos(angles), jnp.sin(angles)], axis=1)

def rope_tables(positions, head_size):
    first_size = head_size // 8
    other_size = (head_size - first_size) // 2
    pieces = []
    swapped = []
    sign_vec = []
    offset = 0
    for axis_id, width_part in enumerate((first_size, other_size, other_size)):
        half_size = width_part // 2
        freq_rate = jnp.exp(-jnp.log(256.0) * 2.0 * jnp.arange(half_size, dtype=jnp.float32) / width_part)
        angle_part = positions[axis_id].astype(jnp.float32)[:, None] * freq_rate[None, :]
        pieces.append(angle_part)
        pieces.append(angle_part)
        swapped += list(range(offset + half_size, offset + width_part)) + list(range(offset, offset + half_size))
        sign_vec += [-1.0] * half_size + [1.0] * half_size
        offset += width_part
    angles = jnp.concatenate(pieces, axis=1)
    return (jnp.cos(angles), jnp.sin(angles), np.array(swapped, np.int32), np.array(sign_vec, np.float32))

def rotate(values, tables):
    cos_tab, sin_tab, swapped, sign_vec = tables
    return values * cos_tab + values[..., swapped] * sign_vec * sin_tab

def unrotate(values, tables):
    cos_tab, sin_tab, swapped, sign_vec = tables
    return values * cos_tab - (values * sin_tab)[..., swapped] * sign_vec

def rms_norm(values):
    inverse = lax.rsqrt(lax.optimization_barrier(jnp.mean(values * values, -1, keepdims=True)) + epsilon)
    return (values * inverse, inverse)

def rms_back(d_normed, normed, inverse):
    return inverse * (d_normed - normed * lax.optimization_barrier(jnp.mean(d_normed * normed, -1, keepdims=True)))

def layer_norm(values):
    centred = values - lax.optimization_barrier(jnp.mean(values, -1, keepdims=True))
    inverse_std = lax.rsqrt(lax.optimization_barrier(jnp.mean(centred * centred, -1, keepdims=True)) + epsilon)
    return (centred * inverse_std, inverse_std)

def layer_norm_back(d_normed, normed, inverse_std):
    return inverse_std * (d_normed - lax.optimization_barrier(jnp.mean(d_normed, -1, keepdims=True)) - normed * lax.optimization_barrier(jnp.mean(d_normed * normed, -1, keepdims=True)))

def attend(projected, tables):
    length, groups, triple = projected.shape
    head_size = triple // 3
    grouped = jnp.transpose(projected.reshape(length, groups, 3, head_size), (2, 1, 0, 3))
    query_n, query_inv = rms_norm(grouped[0])
    key_n, key_inv = rms_norm(grouped[1])
    q_rot = rotate(query_n, tables).astype(jnp.bfloat16)
    k_rot = rotate(key_n, tables).astype(jnp.bfloat16)
    values = grouped[2].astype(jnp.bfloat16)
    score_scale = head_size ** (-0.5)
    scores = jnp.einsum('gld,gmd->glm', q_rot.astype(jnp.float32), k_rot.astype(jnp.float32)) * score_scale
    weights = jnp.exp(scores - head_size ** 0.5)
    probs = weights / lax.optimization_barrier(jnp.sum(weights, -1, keepdims=True))
    probs_low = probs.astype(jnp.bfloat16)
    heads_out = jnp.einsum('glm,gmd->gld', probs_low.astype(jnp.float32), values.astype(jnp.float32))
    attended = jnp.transpose(heads_out, (1, 0, 2)).reshape(length, groups * head_size).astype(jnp.bfloat16)
    saved = (q_rot, k_rot, values, probs, probs_low, query_n, query_inv, key_n, key_inv)
    return (attended, saved)

def attend_back(d_attended, saved, tables):
    q_rot, k_rot, values, probs, probs_low, query_n, query_inv, key_n, key_inv = saved
    groups, length, head_size = q_rot.shape
    score_scale = head_size ** (-0.5)
    d_heads = jnp.transpose(d_attended.reshape(length, groups, head_size), (1, 0, 2)).astype(jnp.float32)
    d_values = jnp.einsum('glm,gld->gmd', probs_low.astype(jnp.float32), d_heads)
    d_probs = jnp.einsum('gld,gmd->glm', d_heads, values.astype(jnp.float32))
    d_scores = (probs * (d_probs - lax.optimization_barrier(jnp.sum(probs * d_probs, -1, keepdims=True)))).astype(jnp.bfloat16)
    d_qrot = jnp.einsum('glm,gmd->gld', d_scores.astype(jnp.float32), k_rot.astype(jnp.float32)) * score_scale
    d_krot = jnp.einsum('glm,gld->gmd', d_scores.astype(jnp.float32), q_rot.astype(jnp.float32)) * score_scale
    d_query = rms_back(unrotate(d_qrot, tables), query_n, query_inv)
    d_key = rms_back(unrotate(d_krot, tables), key_n, key_inv)
    stacked = jnp.stack([d_query, d_key, d_values], 0)
    return jnp.transpose(stacked, (2, 1, 0, 3)).reshape(length, groups * 3 * head_size).astype(jnp.bfloat16)

def reference(latent, timesteps, positions, mod_weight, input_weight, output_weight, cotangent):
    time_act = jax.nn.silu(time_embed(timesteps, D)).astype(jnp.bfloat16)
    modulation = jnp.dot(time_act, mod_weight, preferred_element_type=jnp.float32)
    tables = rope_tables(positions, HEAD)
    flat_in = input_weight.reshape(D, HEADS * 3 * HEAD)
    flat_out = output_weight.reshape(HEADS * HEAD, D)
    group_in = jnp.transpose(input_weight.reshape(D, N_SEQ, GROUP * 3 * HEAD), (1, 0, 2))

    def one_candidate(items):
        latent_one, mod_one, cot_one = items
        shift_vec = mod_one[:D]
        scale_vec = mod_one[D:2 * D]
        gate_vec = mod_one[2 * D:]
        normed, inverse_std = layer_norm(latent_one.astype(jnp.float32))
        modulated = (normed * (1.0 + scale_vec) + shift_vec).astype(jnp.bfloat16)
        projected = jnp.dot(modulated, flat_in, preferred_element_type=jnp.float32)
        attended, saved = attend(projected.reshape(LEN, HEADS, 3 * HEAD), tables)
        mixed = jnp.dot(attended, flat_out, preferred_element_type=jnp.float32)
        block_one = (latent_one.astype(jnp.float32) + gate_vec * mixed).astype(jnp.bfloat16)
        d_mixed = (cot_one.astype(jnp.float32) * gate_vec).astype(jnp.bfloat16)
        d_attended = lax.dot_general(d_mixed, flat_out, (((1,), (1,)), ((), ())), preferred_element_type=jnp.float32).astype(jnp.bfloat16)
        d_projected = attend_back(d_attended, saved, tables)
        d_groups = jnp.transpose(d_projected.reshape(LEN, N_SEQ, GROUP * 3 * HEAD), (1, 0, 2))

        def add_group(total, pieces):
            d_part, w_part = pieces
            partial_sum = lax.dot_general(d_part, w_part, (((1,), (1,)), ((), ())), preferred_element_type=jnp.float32)
            rounded = lax.optimization_barrier(partial_sum.astype(jnp.bfloat16))
            return (total + rounded.astype(jnp.float32), None)
        d_modulated, _unused = lax.scan(add_group, jnp.zeros((LEN, D), jnp.float32), (d_groups, group_in))
        grad_one = cot_one.astype(jnp.float32) + layer_norm_back(d_modulated * (1.0 + scale_vec), normed, inverse_std)
        return (block_one, grad_one)
    block_out, latent_grad = lax.map(one_candidate, (latent, modulation, cotangent))
    return (block_out, latent_grad)
```

```python
import jax
import jax.numpy as jnp
import numpy as np
from jax import lax
from jax.sharding import Mesh
from jax.sharding import PartitionSpec as P

HEAD = 128

epsilon = 1e-06


def shift(value, axis, step):
    size = lax.axis_size(axis)
    return lax.ppermute(value, axis, [(i, (i + step) % size) for i in range(size)])


def time_embed(timesteps, feature_width):
    half_size = feature_width // 2
    freq_rate = jnp.exp(-jnp.log(10000.0) * jnp.arange(half_size, dtype=jnp.float32) / half_size)
    angles = timesteps.astype(jnp.float32)[:, None] * freq_rate[None, :]
    return jnp.concatenate([jnp.cos(angles), jnp.sin(angles)], axis=1)


def rope_tables(positions, head_size):
    first_size = head_size // 8
    other_size = (head_size - first_size) // 2
    pieces = []
    swapped = []
    sign_vec = []
    offset = 0
    for axis_id, width_part in enumerate((first_size, other_size, other_size)):
        half_size = width_part // 2
        freq_rate = jnp.exp(
            -jnp.log(256.0) * 2.0 * jnp.arange(half_size, dtype=jnp.float32) / width_part
        )
        angle_part = positions[axis_id].astype(jnp.float32)[:, None] * freq_rate[None, :]
        pieces.append(angle_part)
        pieces.append(angle_part)
        swapped += list(range(offset + half_size, offset + width_part)) + list(
            range(offset, offset + half_size)
        )
        sign_vec += [-1.0] * half_size + [1.0] * half_size
        offset += width_part
    angles = jnp.concatenate(pieces, axis=1)
    return (
        jnp.cos(angles),
        jnp.sin(angles),
        np.array(swapped, np.int32),
        np.array(sign_vec, np.float32),
    )


def rotate(values, tables):
    cos_tab, sin_tab, swapped, sign_vec = tables
    return values * cos_tab + values[..., swapped] * sign_vec * sin_tab


def unrotate(values, tables):
    cos_tab, sin_tab, swapped, sign_vec = tables
    return values * cos_tab - (values * sin_tab)[..., swapped] * sign_vec


def rms_norm(values):
    inverse = lax.rsqrt(jnp.mean(values * values, -1, keepdims=True) + epsilon)
    return (values * inverse, inverse)


def rms_back(d_normed, normed, inverse):
    return inverse * (d_normed - normed * jnp.mean(d_normed * normed, -1, keepdims=True))


def layer_norm(values):
    centred = values - jnp.mean(values, -1, keepdims=True)
    inverse_std = lax.rsqrt(jnp.mean(centred * centred, -1, keepdims=True) + epsilon)
    return (centred * inverse_std, inverse_std)


def layer_norm_back(d_normed, normed, inverse_std):
    return inverse_std * (
        d_normed
        - jnp.mean(d_normed, -1, keepdims=True)
        - normed * jnp.mean(d_normed * normed, -1, keepdims=True)
    )


def f32_einsum(expr, *args):
    return jnp.einsum(expr, *args, preferred_element_type=jnp.float32)


def attend(projected, tables):
    head_size = HEAD
    query_n, query_inv = rms_norm(projected[:, :head_size].astype(jnp.float32))
    key_n, key_inv = rms_norm(projected[:, head_size : 2 * head_size].astype(jnp.float32))
    q_rot = rotate(query_n, tables).astype(jnp.bfloat16)
    k_rot = rotate(key_n, tables).astype(jnp.bfloat16)
    values = projected[:, 2 * head_size :]
    scores = f32_einsum("ld,md->lm", q_rot, k_rot) * head_size ** (-0.5)
    weights = jnp.exp(scores - head_size**0.5)
    probs = weights / jnp.sum(weights, -1, keepdims=True)
    probs_low = probs.astype(jnp.bfloat16)
    attended = f32_einsum("lm,md->ld", probs_low, values).astype(jnp.bfloat16)
    saved = (q_rot, k_rot, values, probs, probs_low, query_n, query_inv, key_n, key_inv)
    return (attended, saved)


def attend_back(d_heads, saved, tables):
    q_rot, k_rot, values, probs, probs_low, query_n, query_inv, key_n, key_inv = saved
    score_scale = HEAD ** (-0.5)
    d_values = f32_einsum("lm,ld->md", probs_low, d_heads)
    d_probs = f32_einsum("ld,md->lm", d_heads, values)
    d_scores = (probs * (d_probs - jnp.sum(probs * d_probs, -1, keepdims=True))).astype(
        jnp.bfloat16
    )
    d_qrot = f32_einsum("lm,md->ld", d_scores, k_rot) * score_scale
    d_krot = f32_einsum("lm,ld->md", d_scores, q_rot) * score_scale
    d_query = rms_back(unrotate(d_qrot, tables), query_n, query_inv)
    d_key = rms_back(unrotate(d_krot, tables), key_n, key_inv)
    return jnp.concatenate([d_query, d_key, d_values], 1).astype(jnp.bfloat16)


def summed_on_arrival(value, axis):
    parts = lax.all_to_all(value, axis, 0, 0, tiled=True)
    return jnp.sum(parts.astype(jnp.float32), axis=0)


def from_everyone(value, axis):
    copies = jnp.broadcast_to(value, (lax.axis_size(axis), *value.shape))
    return lax.all_to_all(copies, axis, split_axis=0, concat_axis=0, tiled=True)


def near_rows(value):
    return [value] + [shift(value, "y", k) for k in (1, -1, 2)]


def near_sum(value):
    own, *others = jnp.split(value, 4, 0)
    for k, part in zip((-1, 1, 2), others):
        own = own + shift(part.astype(jnp.bfloat16), "y", k).astype(jnp.float32)
    return own


def all_weights(shard):
    half = shard.shape[0] // 2
    zh_at = lax.axis_index("zh")
    x_at = lax.axis_index("x")
    c_at = lax.axis_index("c")
    pieces = []
    for zh, mine in ((zh_at, shard), (1 - zh_at, shift(shard, "zh", 1))):
        own = jnp.stack([mine] + [shift(mine, "zl", r) for r in (1, 2, 3)], 0)
        left = shift(own, "x", 1)
        right = shift(own, "x", -1)
        far_low = shift(left[:, :half], "x", 1)
        far_high = shift(right[:, half:], "x", -1)
        far = jnp.concatenate([far_low, far_high], 1)
        for step, piece in ((0, own), (1, left), (3, right), (2, far)):
            at = zh * 8 + (x_at + 4 - step) % 4 * 2
            pieces.append((at + c_at, piece))
            pieces.append((at + 1 - c_at, shift(piece, "c", 1)))
    return pieces


def placed_rows(pieces, low, top):
    rows = pieces[0][1].shape[1]
    whole = jnp.zeros((4, 16, rows, top - low), jnp.bfloat16)
    for at, piece in pieces:
        whole = lax.dynamic_update_slice(whole, piece[:, None, :, low:top], (0, at, 0, 0))
    return whole.reshape(4, 16 * rows, top - low)


def on_device(latent, timesteps, positions, mod_weight, input_weight, output_weight, cotangent):
    width = latent.shape[2]
    tokens = latent.shape[1]
    cands = ("zh", "x", "c")
    time_act = jax.nn.silu(time_embed(timesteps, width)).astype(jnp.bfloat16)
    slab_rows = mod_weight.shape[0]
    act_rows = lax.dynamic_slice_in_dim(time_act, lax.axis_index(cands) * slab_rows, slab_rows, 1)
    mod_mine = summed_on_arrival(
        jnp.dot(act_rows, mod_weight, preferred_element_type=jnp.float32).astype(jnp.bfloat16), cands
    )
    modulation = from_everyone(mod_mine, ("zl", "y")).reshape(-1)
    shift_vec = modulation[:width]
    scale_vec = modulation[width : 2 * width]
    gate_vec = modulation[2 * width :]

    weights = all_weights(jnp.concatenate([input_weight[:, 0, :], output_weight[0].T], 1))
    w_in = placed_rows(weights, 0, 3 * HEAD)
    w_out = placed_rows(weights, 3 * HEAD, 4 * HEAD)
    near = near_rows(jnp.stack([latent[0], cotangent[0]], 0))
    latent_near = jnp.concatenate([part[0] for part in near], 0).astype(jnp.float32)
    cot_near = jnp.concatenate([part[1] for part in near], 0)

    y_at = lax.axis_index("y")
    z_at = lax.axis_index("zl")
    by_yz = positions.reshape(3, 4, 4, tokens)
    by_yz = jnp.concatenate(
        [lax.dynamic_slice_in_dim(by_yz, (y_at + k) % 4, 1, 2) for k in (0, 3, 1, 2)], 2
    )
    by_yz = jnp.concatenate(
        [lax.dynamic_slice_in_dim(by_yz, (z_at + k) % 4, 1, 1) for k in range(4)], 1
    )
    tables = rope_tables(by_yz.reshape(3, 16 * tokens), HEAD)

    normed_near, inverse_near = layer_norm(latent_near)
    modulated = (normed_near * (1.0 + scale_vec) + shift_vec).astype(jnp.bfloat16)
    d_mixed = (cot_near.astype(jnp.float32) * gate_vec).astype(jnp.bfloat16)

    projected = f32_einsum("tk,hkn->htn", modulated, w_in).astype(jnp.bfloat16)
    d_attended = f32_einsum("tc,hcd->htd", d_mixed, w_out).astype(jnp.bfloat16)
    to_heads = jnp.concatenate([projected, d_attended], 2)
    at_head = jnp.concatenate(
        [to_heads[0]] + [shift(to_heads[r], "zl", -r) for r in (1, 2, 3)], 0
    )
    attended, saved = attend(at_head[:, : 3 * HEAD], tables)
    d_projected = attend_back(at_head[:, 3 * HEAD :], saved, tables)

    def to_tokens(value):
        parts = jnp.split(value, 4, 0)
        return jnp.stack([parts[0]] + [shift(parts[r], "zl", r) for r in (1, 2, 3)], 0)

    mixed = near_sum(f32_einsum("htd,hcd->tc", to_tokens(attended), w_out))
    d_modulated = near_sum(f32_einsum("htn,hkn->tk", to_tokens(d_projected), w_in))
    block_out = (latent[0].astype(jnp.float32) + gate_vec * mixed).astype(jnp.bfloat16)
    latent_grad = cotangent[0].astype(jnp.float32) + layer_norm_back(
        d_modulated * (1.0 + scale_vec), normed_near[:tokens], inverse_near[:tokens]
    )
    return (block_out[None], latent_grad[None])


def solution(mesh):
    fine = Mesh(mesh.devices.reshape(2, 4, 2, 4, 4), ("zh", "x", "c", "zl", "y"))
    cand = ("zh", "x", "c")
    seq = ("zl", "y")
    placed = (
        P(cand, seq, None),
        P(),
        P(),
        P(cand, seq),
        P(cand, seq, None),
        P(seq, None, cand),
        P(cand, seq, None),
    )
    return jax.shard_map(
        on_device,
        mesh=fine,
        in_specs=placed,
        out_specs=(P(cand, seq, None), P(cand, seq, None)),
        check_vma=False,
    )
```

```python
import jax
import jax.numpy as jnp
import numpy as np
from jax import lax
from jax.experimental import pallas as pl
from jax.experimental.pallas import tpu as pltpu
from jax.sharding import Mesh
from jax.sharding import PartitionSpec as P


HEAD = 128

epsilon = 1e-06


def shift(value, axis, step):
    size = lax.axis_size(axis)
    return lax.ppermute(value, axis, [(i, (i + step) % size) for i in range(size)])


def time_embed(timesteps, feature_width):
    half_size = feature_width // 2
    freq_rate = jnp.exp(-jnp.log(10000.0) * jnp.arange(half_size, dtype=jnp.float32) / half_size)
    angles = timesteps.astype(jnp.float32)[:, None] * freq_rate[None, :]
    return jnp.concatenate([jnp.cos(angles), jnp.sin(angles)], axis=1)


def rope_tables(positions, head_size):
    first_size = head_size // 8
    other_size = (head_size - first_size) // 2
    pieces = []
    sign_vec = []
    for axis_id, width_part in enumerate((first_size, other_size, other_size)):
        half_size = width_part // 2
        freq_rate = jnp.exp(
            -jnp.log(256.0) * 2.0 * jnp.arange(half_size, dtype=jnp.float32) / width_part
        )
        angle_part = positions[axis_id].astype(jnp.float32)[:, None] * freq_rate[None, :]
        pieces.append(angle_part)
        pieces.append(angle_part)
        sign_vec += [-1.0] * half_size + [1.0] * half_size
    angles = jnp.concatenate(pieces, axis=1)
    return jnp.cos(angles), jnp.sin(angles) * np.array(sign_vec, np.float32)


def partner(values):
    lane = lax.broadcasted_iota(jnp.int32, values.shape, 1)
    small = jnp.where(lane < 8, pltpu.roll(values, 120, 1), pltpu.roll(values, 8, 1))
    first = (lane < 44) | ((lane >= 72) & (lane < 100))
    large = jnp.where(first, pltpu.roll(values, 100, 1), pltpu.roll(values, 28, 1))
    return jnp.where(lane < 16, small, large)


def rms_norm(values):
    inverse = lax.rsqrt(jnp.mean(values * values, -1, keepdims=True) + epsilon)
    return (values * inverse, inverse)


def rms_back(d_normed, normed, inverse):
    return inverse * (d_normed - normed * jnp.mean(d_normed * normed, -1, keepdims=True))


def dot_f32(left, right, dims):
    return lax.dot_general(left, right, ((dims[:1], dims[1:]), ((), ())), preferred_element_type=jnp.float32)


def layer_norm(values):
    centred = values - jnp.mean(values, -1, keepdims=True)
    inverse_std = lax.rsqrt(jnp.mean(centred * centred, -1, keepdims=True) + epsilon)
    return (centred * inverse_std, inverse_std)


def layer_norm_back(d_normed, normed, inverse_std):
    return inverse_std * (
        d_normed
        - jnp.mean(d_normed, -1, keepdims=True)
        - normed * jnp.mean(d_normed * normed, -1, keepdims=True)
    )


SCALE = HEAD ** (-0.5)
VMEM = pl.BlockSpec(memory_space=pltpu.VMEM)


def attend_kernel(*refs):
    parts, (cos, sin), attended = refs[:4], refs[4:6], refs[6:10]
    q_out, k_out, v_out, probs_out = refs[10:]
    size = parts[0].shape[0]
    for i, part in enumerate(parts):
        rows = pl.ds(i * size, size)
        for at, out in ((0, q_out), (1, k_out)):
            normed, _ = rms_norm(part[:, at * HEAD : (at + 1) * HEAD].astype(jnp.float32))
            turned = normed * cos[rows, :] + partner(normed) * sin[rows, :]
            out[rows, :] = turned.astype(jnp.bfloat16)
        v_out[rows, :] = part[:, 2 * HEAD :]
    for i, out in enumerate(attended):
        rows = pl.ds(i * size, size)
        scores = dot_f32(q_out[rows, :], k_out[...], (1, 1)) * SCALE
        weights = jnp.exp(scores - HEAD**0.5)
        probs = weights / jnp.sum(weights, -1, keepdims=True)
        probs_out[rows, :] = probs
        out[...] = dot_f32(probs.astype(jnp.bfloat16), v_out[...], (1, 0)).astype(jnp.bfloat16)


def attend(qkv, tables):
    size = qkv[0].shape[0]
    length = 4 * size
    shape = jax.ShapeDtypeStruct
    low = shape((length, HEAD), jnp.bfloat16)
    out = pl.pallas_call(
        attend_kernel,
        in_specs=[VMEM] * 6,
        out_specs=[VMEM] * 8,
        out_shape=[shape((size, HEAD), jnp.bfloat16)] * 4
        + [low] * 3
        + [shape((length, length), jnp.float32)],
        cost_estimate=pl.CostEstimate(flops=4 * 10**9, bytes_accessed=4 * 10**6, transcendentals=length * length),
    )(*qkv, *tables)
    return out[:4], out[4:]


def back_kernel(*refs):
    parts, d_heads, (q_rot, k_rot, values, probs_in, cos, sin) = refs[:4], refs[4:8], refs[8:14]
    outs, (d_keys, d_values) = refs[14:18], refs[18:]
    size = parts[0].shape[0]

    def turned_back(turned, at, i):
        rows = pl.ds(i * size, size)
        normed, inverse = rms_norm(parts[i][:, at * HEAD : (at + 1) * HEAD].astype(jnp.float32))
        back = turned * cos[rows, :] - partner(turned) * sin[rows, :]
        outs[i][:, at * HEAD : (at + 1) * HEAD] = rms_back(back, normed, inverse).astype(jnp.bfloat16)

    for i in range(4):
        probs = probs_in[pl.ds(i * size, size), :]
        d_head = d_heads[i][...]
        d_probs = dot_f32(d_head, values[...], (1, 1))
        d_scores = (probs * (d_probs - jnp.sum(probs * d_probs, -1, keepdims=True))).astype(jnp.bfloat16)
        turned_back(dot_f32(d_scores, k_rot[...], (1, 0)) * SCALE, 0, i)
        d_value = dot_f32(probs.astype(jnp.bfloat16), d_head, (0, 0))
        d_key = dot_f32(d_scores, q_rot[pl.ds(i * size, size), :], (0, 0))
        d_values[...] = d_value if i == 0 else d_values[...] + d_value
        d_keys[...] = d_key if i == 0 else d_keys[...] + d_key
    for i in range(4):
        rows = pl.ds(i * size, size)
        turned_back(d_keys[rows, :] * SCALE, 1, i)
        outs[i][:, 2 * HEAD :] = d_values[rows, :].astype(jnp.bfloat16)


def attend_back(d_heads, qkv, saved, tables):
    size = qkv[0].shape[0]
    return pl.pallas_call(
        back_kernel,
        in_specs=[VMEM] * 14,
        out_specs=[VMEM] * 4,
        out_shape=[jax.ShapeDtypeStruct((size, 3 * HEAD), jnp.bfloat16)] * 4,
        scratch_shapes=[pltpu.VMEM((4 * size, HEAD), jnp.float32)] * 2,
        cost_estimate=pl.CostEstimate(flops=6 * 10**9, bytes_accessed=4 * 10**6, transcendentals=0),
    )(*qkv, *d_heads, *saved, *tables)


def cost_of(pieces, rows):
    size = sum(piece.size for piece in pieces)
    return pl.CostEstimate(flops=2 * rows * size, bytes_accessed=2 * size, transcendentals=0)


def weight_copies(pieces, whole, sems):
    heads, rows, cols = pieces[0].shape
    zh_at = lax.axis_index("zh")
    x_at = lax.axis_index("x")
    c_at = lax.axis_index("c")
    copies = [[] for _ in range(4)]
    for i, piece in enumerate(pieces):
        for j in range(heads):
            zh = zh_at if i < 8 and j < 4 else 1 - zh_at
            x = (x_at + (0, 3, 1, 2)[i // 2 % 4]) % 4
            c = c_at if i % 2 == 0 else 1 - c_at
            at = pl.multiple_of((zh * 8 + x * 2 + c) * rows, rows)
            h = j % 4
            place = whole.at[pl.ds(at, rows), pl.ds(h * cols, cols)]
            copies[h].append(pltpu.make_async_copy(piece.at[j], place, sems.at[h, len(copies[h])]))
    return copies


def with_weights(kernel, values, out_shapes, pieces):
    heads, rows, cols = pieces[0].shape
    count = len(pieces)
    blocks = count * heads // 4
    n_in, n_out = len(values), len(out_shapes)

    def body(*refs):
        values, parts, outs = refs[:n_in], refs[n_in : n_in + count], refs[n_in + count : -2]
        whole, sems = refs[-2:]
        copies = weight_copies(parts, whole, sems)
        for head in copies:
            for copy in head:
                copy.start()

        def ready(head):
            for copy in copies[head]:
                copy.wait()

        kernel(ready, values, whole, outs)

    vmem = pl.BlockSpec(memory_space=pltpu.VMEM)
    return pl.pallas_call(
        body,
        in_specs=[vmem] * n_in + [pl.BlockSpec(memory_space=pl.ANY)] * count,
        out_specs=[vmem] * n_out,
        out_shape=[jax.ShapeDtypeStruct(shape, jnp.bfloat16) for shape in out_shapes],
        scratch_shapes=[
            pltpu.VMEM((blocks * rows, 4 * cols), jnp.bfloat16),
            pltpu.SemaphoreType.DMA((4, blocks)),
        ],
        cost_estimate=cost_of(pieces, values[0].shape[0]),
    )(*values, *pieces)


def times_weights(value, pieces):
    tokens = value.shape[0]
    cols = pieces[0].shape[2]

    def kernel(ready, values, whole, outs):
        for first in (2, 0):
            ready(first)
            ready(first + 1)
            both = dot_f32(values[0][...], whole[:, first * cols : (first + 2) * cols], (1, 0))
            both = both.astype(jnp.bfloat16)
            outs[first][...] = both[:, :cols]
            outs[first + 1][...] = both[:, cols:]

    return with_weights(kernel, [value], [(tokens, cols)] * 4, pieces)


def times_weights_back(values, pieces):
    tokens = values[0].shape[0]
    heads, rows, _ = pieces[0].shape
    part = tokens // 4

    def kernel(ready, values, whole, outs):
        for head in range(4):
            ready(head)
        both = jnp.concatenate([value[...] for value in values], 1)
        total = dot_f32(both, whole[...], (1, 1)).astype(jnp.bfloat16)
        for i in range(4):
            outs[i][...] = total[i * part : (i + 1) * part]

    width = len(pieces) * heads // 4 * rows
    return with_weights(kernel, values, [(part, width)] * 4, pieces)


def summed_on_arrival(value, axis):
    parts = lax.all_to_all(value, axis, 0, 0, tiled=True)
    return jnp.sum(parts.astype(jnp.float32), axis=0)


def from_everyone(value, axis):
    copies = jnp.broadcast_to(value, (lax.axis_size(axis), *value.shape))
    return lax.all_to_all(copies, axis, split_axis=0, concat_axis=0, tiled=True)


def near_rows(value):
    return [value] + [shift(value, "y", k) for k in (1, -1, 2)]


def near_sum(value):
    total = value[0].astype(jnp.float32)
    for k, part in zip((-1, 1, 2), value[1:]):
        total = total + shift(part, "y", k).astype(jnp.float32)
    return total


def along_x(own):
    half = own.shape[1] // 2
    left = shift(own, "x", 1)
    right = shift(own, "x", -1)
    far_low = shift(left[:, :half], "x", 1)
    far_high = shift(right[:, half:], "x", -1)
    far = jnp.concatenate([far_low, far_high], 1)
    pieces = []
    for piece in (own, left, right, far):
        pieces += [piece, shift(piece, "c", 1)]
    return pieces


def all_weights(shard_in, shard_out):
    shard = jnp.concatenate([shard_in, shard_out], 1)
    near = jnp.stack([shard] + [shift(shard, "zl", r) for r in (1, 3, 2)], 0)
    across = shift(shard, "zh", 1)
    far = jnp.stack([across] + [shift(across, "zl", r) for r in (1, 3, 2)], 0)
    split = 3 * HEAD
    for_in = along_x(near[:, :, :split]) + along_x(far[:, :, :split])
    for_out = along_x(jnp.concatenate([near[:, :, split:], far[:, :, split:]], 0))
    return for_in, for_out


HEADS_AT = (0, 1, 3, 2)


def to_heads(value):
    return [value[0], *(shift(value[i], "zl", -HEADS_AT[i]) for i in (1, 2, 3))]


def to_tokens(value):
    return [value[0], *(shift(value[i], "zl", HEADS_AT[i]) for i in (1, 2, 3))]


def on_device_body(latent, timesteps, positions, mod_weight, input_weight, output_weight, cotangent):
    width = latent.shape[2]
    tokens = latent.shape[1]
    cands = ("zh", "x", "c")
    w_in, w_out = all_weights(input_weight[:, 0, :], output_weight[0].T)

    time_act = jax.nn.silu(time_embed(timesteps, width)).astype(jnp.bfloat16)
    slab_rows = mod_weight.shape[0]
    act_rows = lax.dynamic_slice_in_dim(time_act, lax.axis_index(cands) * slab_rows, slab_rows, 1)
    partial = jnp.dot(act_rows, mod_weight, preferred_element_type=jnp.float32).astype(jnp.bfloat16)
    mod_mine = summed_on_arrival(partial, cands)
    modulation = from_everyone(mod_mine, ("zl", "y")).reshape(-1)
    shift_vec = modulation[:width]
    scale_vec = modulation[width : 2 * width]
    gate_vec = modulation[2 * width :]

    near = near_rows(jnp.concatenate([latent[0], cotangent[0]], 0))
    latent_near = jnp.concatenate([part[:tokens] for part in near], 0).astype(jnp.float32)
    cot_near = jnp.concatenate([part[tokens:] for part in near], 0)

    y_at = lax.axis_index("y")
    z_at = lax.axis_index("zl")
    by_yz = positions.reshape(3, 4, 4, tokens)
    by_yz = jnp.concatenate(
        [lax.dynamic_slice_in_dim(by_yz, (y_at + k) % 4, 1, 2) for k in (0, 3, 1, 2)], 2
    )
    by_yz = jnp.concatenate(
        [lax.dynamic_slice_in_dim(by_yz, (z_at + k) % 4, 1, 1) for k in HEADS_AT], 1
    )
    tables = rope_tables(by_yz.reshape(3, 16 * tokens), HEAD)

    normed_near, inverse_near = layer_norm(latent_near)
    modulated = (normed_near * (1.0 + scale_vec) + shift_vec).astype(jnp.bfloat16)
    d_mixed = (cot_near.astype(jnp.float32) * gate_vec).astype(jnp.bfloat16)

    qkv = to_heads(times_weights(modulated, w_in))
    d_heads = to_heads(times_weights(d_mixed, w_out))
    attended, saved = attend(qkv, tables)
    mixed = times_weights_back(to_tokens(attended), w_out)
    d_qkv = attend_back(d_heads, qkv, saved, tables)
    d_modulated = times_weights_back(to_tokens(d_qkv), w_in)
    mixed = near_sum(mixed)
    d_modulated = near_sum(d_modulated)
    block_out = (latent[0].astype(jnp.float32) + gate_vec * mixed).astype(jnp.bfloat16)
    latent_grad = cotangent[0].astype(jnp.float32) + layer_norm_back(
        d_modulated * (1.0 + scale_vec), normed_near[:tokens], inverse_near[:tokens]
    )
    return (block_out[None], latent_grad[None])


def solution(mesh):
    fine = Mesh(mesh.devices.reshape(2, 4, 2, 4, 4), ("zh", "x", "c", "zl", "y"))
    cand = ("zh", "x", "c")
    seq = ("zl", "y")
    placed = (
        P(cand, seq, None),
        P(),
        P(),
        P(cand, seq),
        P(cand, seq, None),
        P(seq, None, cand),
        P(cand, seq, None),
    )
    return jax.shard_map(
        on_device_body,
        mesh=fine,
        in_specs=placed,
        out_specs=(P(cand, seq, None), P(cand, seq, None)),
        check_vma=False,
    )
```
